32 devices in a mesh: tensor: 4 (over y, core), context: 8 (over z, x).
Axes of the slice: x: 2, y: 2, z: 4, core: 2. Of those that a mesh axis runs over, the one named last changes fastest.
Arguments:
- tokens: bfloat16 [2048, 5120], P('context', 'tensor'), may hold values from -6 to 6
- query_weight: bfloat16 [5120, 5120], P('context', 'tensor'), may hold values from -0.078125 to 0.078125
- key_weight: bfloat16 [5120, 5120], P('context', 'tensor'), may hold values from -0.078125 to 0.078125
- value_weight: bfloat16 [5120, 5120], P('context', 'tensor'), may hold values from -0.078125 to 0.078125
- cache_keys: bfloat16 [256, 64, 5120], P('context', None, 'tensor'), may hold values from -160 to 160
- cache_values: bfloat16 [256, 64, 5120], P('context', None, 'tensor'), may hold values from -6 to 6
- selected: int32 [16, 32], P('context'), may hold values from -1 to 255, as said below
- counts: int32 [16], P('context'), may hold values from 24 to 32, as said below
- block_slot: int32 [256], replicated, may hold values from 0 to 255, as said below
Outputs:
- attended: bfloat16 [2048, 5120], P('context', 'tensor')
The draws below stay inside these ranges and needn't reach their ends.
Inputs may be any that keep to these rules, and one draw needn't show every extreme that they name: `selected`: row c names different block ids in its first counts[c] entries and -1 in the others. Among the valid entries of the 2 query blocks of one context device, at most 16 name blocks stored on one context device (block_slot[b] // 32), and exactly 16 do for some device in every draw. `counts`: some query block has 32 valid entries in every draw. `block_slot`: each row of the cache arrays stores exactly one block id.
All inputs are finite; a program needn't handle non-finite values.
Results may differ from the reference program's by a relative error of at most 0.012.
The reference program's roundings to bfloat16 on the way (of `queries` and `weights`) count: a program that leaves them out, or rounds other values in their place, can miss the bound.
Values may be sent and summed in bfloat16 or wider, within the bound.
No kernel may reach another device: no remote copies, remote signals or barrier semaphores. Data moves between devices by JAX's collectives and lax.ppermute only.
A program may use at most 192 MiB of HBM per device.

```python
import jax
import jax.numpy as jnp
from jax import lax

D = 5120
HEADS = 40
HDIM = 128
BLK_DEV = 32
SPAN = 128
BLOCK = 64
SELECT = 32
SPAN_DEV = 2
SPANS = 16
TOKENS = 2048
BLOCKS = 256
OWNERS = 8
CAP = 16


def make_plan(key):
    per_device = SPAN_DEV * SELECT
    tickets = OWNERS * CAP
    seed_perm = jax.random.fold_in(key, 101)
    seed_count = jax.random.fold_in(key, 102)
    seed_busy = jax.random.fold_in(key, 103)
    seed_device = jax.random.fold_in(key, 104)
    seed_full = jax.random.fold_in(key, 105)
    placement_map = jax.random.permutation(seed_perm, BLOCKS).astype(jnp.int32)
    inverse = jnp.argsort(placement_map).astype(jnp.int32)
    counts = jax.random.randint(seed_count, (OWNERS, SPAN_DEV), 3 * SELECT // 4, SELECT + 1).astype(jnp.int32)
    full_device = jax.random.randint(seed_full, (), 0, OWNERS)
    counts = counts.at[full_device, 0].set(SELECT)
    valid_rows = (jnp.arange(SELECT)[None, None, :] < counts[:, :, None]).reshape(OWNERS, per_device)
    busy_owner = jax.random.randint(seed_busy, (OWNERS,), 0, OWNERS)

    def device_plan(device_seed, busiest, valid_row):
        seed_shuffle = jax.random.fold_in(device_seed, 1)
        seed_priority = jax.random.fold_in(device_seed, 2)
        seed_local = jax.random.fold_in(device_seed, 3)
        shuffle = jax.random.permutation(seed_shuffle, tickets)
        ticket_owner = jnp.arange(tickets) // CAP
        ranking = jnp.where(ticket_owner == busiest, shuffle, shuffle + tickets)
        ticket_order = jnp.argsort(ranking)
        priority = jax.random.permutation(seed_priority, per_device)
        second = jnp.where(valid_row, priority, priority + per_device)
        entry_rank = jnp.argsort(jnp.argsort(second))
        ticket_pick = ticket_order[jnp.minimum(entry_rank, tickets - 1)]
        owner_pick = ticket_pick // CAP
        within = ticket_pick % CAP
        local_tables = jax.vmap(lambda owner_seed: jax.random.permutation(owner_seed, BLK_DEV))(jax.random.split(seed_local, OWNERS))
        local_row = local_tables[owner_pick, within]
        return (owner_pick * BLK_DEV + local_row).astype(jnp.int32)
    slot_rows = jax.vmap(device_plan)(jax.random.split(seed_device, OWNERS), busy_owner, valid_rows)
    block_ids = inverse[slot_rows]
    chosen = jnp.where(valid_rows, block_ids, -1).reshape(SPANS, SELECT).astype(jnp.int32)
    return (placement_map, counts.reshape(SPANS), chosen)


def draw_selected(key, part):
    return make_plan(key)[2]


def draw_counts(key, part):
    return make_plan(key)[1]


def draw_block_slot(key, part):
    return make_plan(key)[0]


def draw_cache_keys(key, part):
    seed_normal = jax.random.fold_in(key, 201)
    normal_part = jnp.clip(jax.random.normal(seed_normal, (BLOCKS, BLOCK, HEADS * HDIM), jnp.float32), -4.0, 4.0)
    return normal_part.astype(jnp.bfloat16)


def level_of(key, dims, cuts, low, top_value):
    def one(dim, shards_of):
        heights = jax.random.uniform(jax.random.fold_in(jax.random.fold_in(key, 6), dim), (shards_of,), jnp.float32, low / len(cuts), top_value / len(cuts))
        return jnp.repeat(jnp.exp(heights), dims[dim] // shards_of).reshape((-1,) + (1,) * (len(dims) - dim - 1))

    loudness = one(*cuts[0])
    for cut in cuts[1:]:
        loudness = loudness * one(*cut)
    return loudness


def bell_draw(key, shape, scale, limit, cuts=(), kind=jnp.bfloat16):
    values = scale * jax.random.normal(key, shape, jnp.float32)
    if cuts:
        values = values * level_of(key, shape, cuts, -0.22, 0.18)
    return jnp.clip(values, -limit, limit).astype(kind)


def setup_inputs(seed: int = 0) -> dict:
    seeds = jax.random.split(jax.random.key(seed), 10)
    return {
        "tokens": bell_draw(seeds[0], (TOKENS, D), 1.0, 6.0, ((0, 8), (1, 4))),
        "query_weight": bell_draw(seeds[1], (D, HEADS * HDIM), D ** -0.5, 0.078125, ((0, 8), (1, 4))),
        "key_weight": bell_draw(seeds[2], (D, HEADS * HDIM), D ** -0.5, 0.078125, ((0, 8), (1, 4))),
        "value_weight": bell_draw(seeds[3], (D, HEADS * HDIM), D ** -0.5, 0.078125, ((0, 8), (1, 4))),
        "cache_keys": draw_cache_keys(jax.random.fold_in(seeds[9], 71), 0),
        "cache_values": bell_draw(seeds[5], (BLOCKS, BLOCK, HEADS * HDIM), 1.0, 6.0, ((0, 8), (2, 4))),
        "selected": draw_selected(jax.random.fold_in(seeds[9], 71), 0),
        "counts": draw_counts(jax.random.fold_in(seeds[9], 71), 0),
        "block_slot": draw_block_slot(jax.random.fold_in(seeds[9], 71), 0),
    }


NEGATIVE = -1.0e30


def reference(tokens, query_weight, key_weight, value_weight, cache_keys, cache_values, selected, counts, block_slot):
    head_width = HEADS * HDIM
    score_scale = HDIM ** -0.5
    queries = jnp.dot(tokens, query_weight, preferred_element_type=jnp.float32).astype(jnp.bfloat16)
    new_keys = jnp.dot(tokens, key_weight, preferred_element_type=jnp.float32).astype(jnp.bfloat16)
    new_values = jnp.dot(tokens, value_weight, preferred_element_type=jnp.float32).astype(jnp.bfloat16)
    query_spans = queries.reshape(SPANS, SPAN, HEADS, HDIM)
    key_spans = new_keys.reshape(SPANS, SPAN, head_width)
    value_spans = new_values.reshape(SPANS, SPAN, head_width)
    blank = jnp.zeros((1, SPAN, head_width), jnp.bfloat16)
    prior_keys = jnp.concatenate([blank, key_spans[:-1]], 0)
    prior_values = jnp.concatenate([blank, value_spans[:-1]], 0)
    position = jnp.arange(SPAN)
    causal = position[None, :] <= position[:, None]
    entry_index = jnp.arange(SELECT)

    def one_span(packed):
        span_index, chosen, live_count, query_block, prior_key_block, own_key_block, prior_value_block, own_value_block = packed
        slot_rows = block_slot[jnp.clip(chosen, 0, BLOCKS - 1)]
        far_keys = cache_keys[slot_rows].reshape(SELECT * BLOCK, head_width)
        far_values = cache_values[slot_rows].reshape(SELECT * BLOCK, head_width)
        all_keys = jnp.concatenate([far_keys, prior_key_block, own_key_block], 0).astype(jnp.float32).reshape(-1, HEADS, HDIM)
        all_values = jnp.concatenate([far_values, prior_value_block, own_value_block], 0).astype(jnp.float32).reshape(-1, HEADS, HDIM)
        scores = jnp.einsum("qhd,khd->hqk", query_block.astype(jnp.float32), all_keys) * score_scale
        far_open = jnp.repeat(entry_index < live_count, BLOCK)
        allowed = jnp.concatenate([
            jnp.broadcast_to(far_open[None, :], (SPAN, SELECT * BLOCK)),
            jnp.broadcast_to(span_index > 0, (SPAN, SPAN)),
            causal], 1)
        masked = jnp.where(allowed[None], scores, NEGATIVE)
        highest = jnp.max(masked, axis=2, keepdims=True)
        weights = jnp.where(allowed[None], jnp.exp(masked - highest), 0.0)
        totals = jnp.sum(weights, axis=2)
        rounded = lax.optimization_barrier(weights.astype(jnp.bfloat16)).astype(jnp.float32)
        summed = jnp.einsum("hqk,khd->qhd", rounded, all_values)
        return (summed / jnp.transpose(totals)[:, :, None]).astype(jnp.bfloat16).reshape(SPAN, head_width)

    attended = lax.map(one_span, (jnp.arange(SPANS), selected, counts, query_spans, prior_keys, key_spans, prior_values, value_spans))
    return attended.reshape(TOKENS, head_width)
```

```python
import functools
import math

import jax
import jax.numpy as jnp
from jax import lax
from jax.experimental import pallas as pl
from jax.experimental.pallas import tpu as pltpu
from jax.sharding import PartitionSpec as P

HDIM = 128
LANES = 128
GROUP = 4
STAT_STEP = 32
NEGATIVE = -1e30
SCORE_SCALE = HDIM ** (-0.5)
LOG2E = math.log2(math.e)
BASE2_SCALE = SCORE_SCALE * LOG2E
VMEM_LIMIT = 56 * 1024 * 1024


def params():
    return pltpu.CompilerParams(vmem_limit_bytes=VMEM_LIMIT)


class Grid:
    def __init__(self, tensor, context):
        x_size = max(1, tensor // 2)
        if context % (2 * x_size):
            x_size = 1
        self.T, self.C, self.X = tensor, context, x_size
        self.Z = context // x_size
        self.ZL = self.Z // 2

    def at(self, z, x):
        return (z % self.Z) * self.X + x % self.X

    def move(self, array, target):
        pairs = [(i, target(i // self.X, i % self.X)) for i in range(self.C)]
        return lax.ppermute(array, "context", pairs)

    def shift_x(self, array, step):
        return self.move(array, lambda z, x: self.at(z, x + step))

    def shift_z(self, array, step):
        return self.move(array, lambda z, x: self.at(z + step, x))

    def shift_zl(self, array, step):
        zl = self.ZL
        return self.move(array, lambda z, x: self.at(z // zl * zl + (z % zl + step) % zl, x))

    def swap_half(self, array):
        return self.shift_z(array, self.ZL)


def spread_tokens(grid, tokens):
    T, C, X, ZL = grid.T, grid.C, grid.X, grid.ZL
    half_t = T // 2
    rows, width = tokens.shape
    pairs = []
    for t in range(T):
        for c in range(C):
            z, x = c // X, c % X
            half, low = z // ZL, z % ZL
            goal_t = half * half_t + t % half_t
            goal_c = ((t // half_t) * ZL + low) * X + x
            pairs.append((t * C + c, goal_t * C + goal_c))
    mine = lax.ppermute(tokens, ("tensor", "context"), pairs)
    t = lax.axis_index("tensor")
    y, core = t // 2, t % 2
    y_size = T // 2
    found = []
    for dy in range(y_size):
        block = mine if dy == 0 else lax.ppermute(
            mine, "tensor", [(i, ((i // 2 + dy) % y_size) * 2 + i % 2) for i in range(T)]
        )
        twin = lax.ppermute(block, "tensor", [(i, i ^ 1) for i in range(T)])
        found.append(((y - dy) % y_size * 2 + core, block))
        found.append(((y - dy) % y_size * 2 + 1 - core, twin))
    whole = jnp.zeros((2, rows, half_t * width), tokens.dtype)
    for source, block in found:
        whole = lax.dynamic_update_slice(
            whole, block[None], (source // half_t, 0, source % half_t * width)
        )
    return whole


def gather_weight(grid, weight):
    rows = weight.shape[0]
    cut = max(LANES, rows // 2 // LANES * LANES)
    top, low = weight[:cut], weight[cut:]
    blocks = {(0, 0): [weight]}
    for dx in range(1, grid.X):
        blocks[(0, dx)] = [grid.shift_x(top, dx), grid.shift_x(low, dx)]
    for dz in range(1, grid.ZL):
        near_low = grid.shift_zl(low, dz)
        near_top = grid.shift_zl(top, dz)
        blocks[(dz, 0)] = [near_top, near_low]
        for dx in range(1, grid.X):
            blocks[(dz, dx)] = [
                grid.shift_zl(blocks[(0, dx)][0], dz),
                grid.shift_x(near_low, dx),
            ]
    return blocks


def project_body(piece_counts, *refs):
    n = len(piece_counts)
    total = None
    at = n
    for index in range(n):
        start = 0
        for _ in range(piece_counts[index]):
            w_ref = refs[at]
            at += 1
            depth = w_ref.shape[0]
            part = jnp.dot(
                refs[index][:, start : start + depth], w_ref[...], preferred_element_type=jnp.float32
            )
            start += depth
            total = part if total is None else total + part
    refs[at][...] = total.astype(refs[at].dtype)


def project(features, pieces, out_type):
    rows = features[0].shape[0]
    columns = pieces[0][0].shape[1]
    tile = 256 if columns % 256 == 0 else LANES
    flat = [w for block in pieces for w in block]
    depth = sum(w.shape[0] for w in flat)
    return pl.pallas_call(
        functools.partial(project_body, tuple(len(block) for block in pieces)),
        grid=(columns // tile,),
        in_specs=[pl.BlockSpec(f.shape, lambda j: (0, 0)) for f in features]
        + [pl.BlockSpec((w.shape[0], tile), lambda j: (0, j)) for w in flat],
        out_specs=pl.BlockSpec((rows, tile), lambda j: (0, j)),
        out_shape=jax.ShapeDtypeStruct((rows, columns), out_type),
        compiler_params=params(),
        cost_estimate=pl.CostEstimate(
            flops=2 * rows * depth * columns,
            bytes_accessed=2 * depth * (columns + rows) + 4 * rows * columns,
            transcendentals=0,
        ),
        name="project",
    )(*features, *flat)


def code_stats(stats):
    high = stats.astype(jnp.bfloat16).astype(jnp.float32)
    rest = stats - high
    middle = rest.astype(jnp.bfloat16).astype(jnp.float32)
    low = (rest - middle).astype(jnp.bfloat16).astype(jnp.float32)
    return (high + pltpu.roll(middle, STAT_STEP, 1) + pltpu.roll(low, 2 * STAT_STEP, 1)).astype(
        jnp.bfloat16
    )


def read_stats(coded):
    coded = coded.astype(jnp.float32)
    return (
        coded
        + pltpu.roll(coded, LANES - STAT_STEP, 1)
        + pltpu.roll(coded, LANES - 2 * STAT_STEP, 1)
    )


def write_partial(out_ref, rows, head_count, peak_of, both_of):
    lane = lax.broadcasted_iota(jnp.int32, (rows.size, LANES), 1)
    stats = jnp.zeros((rows.size, LANES), jnp.float32)
    for h in range(head_count):
        both = both_of(h)
        total = both[:, HDIM:]
        live = total > 0.0
        safe = jnp.where(live, total, 1.0)
        out_ref[rows, h * HDIM : (h + 1) * HDIM] = (both[:, :HDIM] / safe).astype(out_ref.dtype)
        log_sum = jnp.where(live, peak_of(h) * BASE2_SCALE + jnp.log2(safe), NEGATIVE)
        stats = jnp.where(lane == h, log_sum, stats)
    out_ref[rows, head_count * HDIM :] = code_stats(stats)


def far_body(item_count, table_ref, source_ref, q_ref, *refs):
    keys, values = refs[:GROUP], refs[GROUP : 2 * GROUP]
    out_ref, peak_ref, both_ref = refs[2 * GROUP :]
    head_count = q_ref.shape[1] // HDIM
    row_count = q_ref.shape[0]
    block_rows = keys[0].shape[1]
    base = (source_ref[0] * item_count + pl.program_id(0)) * 8
    live = table_ref[base + 1]

    @pl.when(table_ref[base + 2] > 0)
    def _():
        peak_ref[...] = jnp.full(peak_ref.shape, NEGATIVE, jnp.float32)
        both_ref[...] = jnp.zeros(both_ref.shape, jnp.float32)

    @pl.when(live > 0)
    def _():
        lane = lax.broadcasted_iota(jnp.int32, (row_count, GROUP * block_rows), 1)
        open_keys = lane < live * block_rows
        ones = jnp.ones((GROUP * block_rows, HDIM), jnp.bfloat16)
        for h in range(head_count):
            part = slice(h * HDIM, (h + 1) * HDIM)
            key = jnp.concatenate([k[0, :, part] for k in keys], 0)
            value = jnp.concatenate([v[0, :, part] for v in values], 0)
            scores = lax.dot_general(
                q_ref[:, part], key, (((1,), (1,)), ((), ())), preferred_element_type=jnp.float32
            )
            scores = jnp.where(open_keys, scores, NEGATIVE)
            before = peak_ref[h]
            peak = jnp.maximum(before, jnp.max(scores, axis=1, keepdims=True))
            fade = jnp.exp2((before - peak) * BASE2_SCALE)
            weights = jnp.exp2((scores - peak[:, :1]) * BASE2_SCALE).astype(jnp.bfloat16)
            grown = jnp.dot(
                weights, jnp.concatenate([value, ones], 1), preferred_element_type=jnp.float32
            )
            peak_ref[h] = peak
            both_ref[h] = both_ref[h] * jnp.concatenate([fade, fade], 1) + grown

    @pl.when(table_ref[base + 3] > 0)
    def _():
        write_partial(
            out_ref, pl.ds(0, row_count), head_count, lambda h: peak_ref[h], lambda h: both_ref[h]
        )


def far_partial(queries, source, table, item_count, cache_keys, cache_values, span_rows):
    rows, width = queries.shape
    head_count = width // HDIM
    block_rows = cache_keys.shape[1]

    def field(i, tab, src, which):
        return tab[(src[0] * item_count + i) * 8 + which]

    def span_map(i, tab, src):
        return (field(i, tab, src, 0), 0)

    def row_map(g):
        return lambda i, tab, src: (field(i, tab, src, 4 + g), 0, 0)

    block_specs = [pl.BlockSpec((1, block_rows, width), row_map(g)) for g in range(GROUP)]
    return pl.pallas_call(
        functools.partial(far_body, item_count),
        grid_spec=pltpu.PrefetchScalarGridSpec(
            num_scalar_prefetch=2,
            grid=(item_count,),
            in_specs=[pl.BlockSpec((span_rows, width), span_map)] + block_specs + block_specs,
            out_specs=pl.BlockSpec((span_rows, width + LANES), span_map),
            scratch_shapes=[
                pltpu.VMEM((head_count, span_rows, HDIM), jnp.float32),
                pltpu.VMEM((head_count, span_rows, 2 * HDIM), jnp.float32),
            ],
        ),
        out_shape=jax.ShapeDtypeStruct((rows, width + LANES), jnp.bfloat16),
        compiler_params=params(),
        cost_estimate=pl.CostEstimate(
            flops=4 * rows * width * GROUP * block_rows * 8,
            bytes_accessed=2 * GROUP * block_rows * width * 2 * item_count,
            transcendentals=rows * head_count * GROUP * block_rows,
        ),
        name="far",
    )(table, source, queries, *([cache_keys] * GROUP), *([cache_values] * GROUP))


def near_body(first_ref, q_ref, k_ref, v_ref, pk_ref, pv_ref, out_ref):
    rows, width = q_ref.shape
    span_rows = pk_ref.shape[0]
    head_count = width // HDIM
    row = lax.broadcasted_iota(jnp.int32, (span_rows, 2 * span_rows), 0)
    lane = lax.broadcasted_iota(jnp.int32, (span_rows, 2 * span_rows), 1)
    causal = lane - span_rows <= row
    ones = jnp.ones((2 * span_rows, HDIM), jnp.bfloat16)
    for j in range(rows // span_rows):
        here = pl.ds(j * span_rows, span_rows)
        opened = causal if j else causal & (lane >= first_ref[0])
        peaks, boths = [], []
        for h in range(head_count):
            part = slice(h * HDIM, (h + 1) * HDIM)
            if j:
                both_rows = pl.ds((j - 1) * span_rows, 2 * span_rows)
                key, value = k_ref[both_rows, part], v_ref[both_rows, part]
            else:
                key = jnp.concatenate([pk_ref[:, part], k_ref[:span_rows, part]], 0)
                value = jnp.concatenate([pv_ref[:, part], v_ref[:span_rows, part]], 0)
            scores = lax.dot_general(
                q_ref[here, part], key, (((1,), (1,)), ((), ())), preferred_element_type=jnp.float32
            )
            scores = jnp.where(opened, scores, NEGATIVE)
            peak = jnp.max(scores, axis=1, keepdims=True)
            weights = jnp.exp2((scores - peak) * BASE2_SCALE).astype(jnp.bfloat16)
            peaks.append(peak)
            boths.append(
                jnp.dot(weights, jnp.concatenate([value, ones], 1), preferred_element_type=jnp.float32)
            )
        write_partial(
            out_ref, here, head_count,
            lambda h: jnp.broadcast_to(peaks[h], (span_rows, LANES)), lambda h: boths[h],
        )


def near_partial(queries, new_keys, new_values, prior_keys, prior_values, first):
    rows, width = queries.shape
    whole = pl.BlockSpec(memory_space=pltpu.VMEM)
    return pl.pallas_call(
        near_body,
        in_specs=[pl.BlockSpec(memory_space=pltpu.SMEM)] + [whole] * 5,
        out_specs=whole,
        out_shape=jax.ShapeDtypeStruct((rows, width + LANES), jnp.bfloat16),
        compiler_params=params(),
        cost_estimate=pl.CostEstimate(
            flops=4 * rows * width * prior_keys.shape[0] * 8,
            bytes_accessed=10 * rows * width,
            transcendentals=rows * width,
        ),
        name="near",
    )(first, queries, new_keys, new_values, prior_keys, prior_values)


def merge_body(count, coded, *refs):
    out_ref = refs[count]
    width = refs[0].shape[1] - LANES
    stats = [read_stats(refs[i][:, width:]) for i in range(count)]
    peak = functools.reduce(jnp.maximum, stats)
    shares = [jnp.exp2(s - peak) for s in stats]
    total = functools.reduce(jnp.add, shares)
    shares = [s / total for s in shares]
    for h in range(width // HDIM):
        part = slice(h * HDIM, (h + 1) * HDIM)
        summed = None
        for i in range(count):
            term = refs[i][:, part].astype(jnp.float32) * shares[i][:, h : h + 1]
            summed = term if summed is None else summed + term
        out_ref[:, part] = summed.astype(out_ref.dtype)
    if coded:
        lane = lax.broadcasted_iota(jnp.int32, peak.shape, 1)
        log_sum = jnp.where(lane < width // HDIM, peak + jnp.log2(total), 0.0)
        out_ref[:, width:] = code_stats(log_sum)


def merge(partials, coded):
    rows, full = partials[0].shape
    width = full if coded else full - LANES
    tile = rows // 2
    return pl.pallas_call(
        functools.partial(merge_body, len(partials), coded),
        grid=(2,),
        in_specs=[pl.BlockSpec((tile, full), lambda i: (i, 0))] * len(partials),
        out_specs=pl.BlockSpec((tile, width), lambda i: (i, 0)),
        out_shape=jax.ShapeDtypeStruct((rows, width), jnp.bfloat16),
        compiler_params=params(),
        cost_estimate=pl.CostEstimate(
            flops=rows * full * 4 * len(partials) * 64,
            bytes_accessed=2 * rows * full * (len(partials) + 1),
            transcendentals=rows * LANES * len(partials),
        ),
        name="merge",
    )(*partials)


def work_table(selected, counts, block_slot, stored, capacity, place):
    spans, select = selected.shape
    packed = jnp.concatenate([selected, counts[:, None]], 1)
    packed = lax.all_gather(packed, "context", axis=0, tiled=True)
    chosen, live_count = packed[:, :select], packed[:, select:]
    entry = jnp.arange(select)
    match = chosen[:, :, None] == jnp.arange(block_slot.shape[0])[None, None, :]
    slot = jnp.sum(jnp.where(match, block_slot[None, None, :], 0), axis=2)
    mine = (entry[None, :] < live_count) & (slot // stored == place)
    earlier = entry[None, :] < entry[:, None]
    rank = jnp.sum(jnp.where(mine[:, None, :] & earlier[None], 1, 0), axis=2)
    position = jnp.arange(capacity)
    hits = mine[:, :, None] & (rank[:, :, None] == position[None, None, :])
    rows = jnp.sum(jnp.where(hits, (slot % stored)[:, :, None], 0), axis=1)
    rows = rows.reshape(-1, spans, capacity)
    held = jnp.sum(jnp.where(mine, 1, 0), axis=1).reshape(-1, spans)
    groups = jnp.maximum(1, (held + GROUP - 1) // GROUP)
    ends = jnp.cumsum(groups, axis=1)
    item_count = capacity // GROUP + spans - 1
    item = jnp.arange(item_count)[None, :]
    active = item < ends[:, -1:]
    item = jnp.minimum(item, ends[:, -1:] - 1)
    span = jnp.sum(jnp.where(item[:, :, None] >= ends[:, None, :], 1, 0), axis=2)
    own = span[:, :, None] == jnp.arange(spans)[None, None, :]
    pick = lambda a: jnp.sum(jnp.where(own, a[:, None, :], 0), axis=2)
    chunk = item - pick(ends - groups)
    live = jnp.where(active, jnp.clip(pick(held) - chunk * GROUP, 0, GROUP), 0)
    first = jnp.where(active & (chunk == 0), 1, 0)
    last = jnp.where(active & (chunk == pick(groups) - 1), 1, 0)
    fields = [span, live, first, last]
    for g in range(GROUP):
        wanted = (chunk * GROUP + g)[:, :, None, None] == position[None, None, None, :]
        fields.append(
            jnp.sum(jnp.where(own[..., None] & wanted, rows[:, None], 0), axis=(2, 3))
        )
    return jnp.stack(fields, axis=2).astype(jnp.int32).reshape(-1), item_count


def shards(
    tokens, query_weight, key_weight, value_weight, cache_keys, cache_values, selected, counts, block_slot
):
    grid = Grid(lax.axis_size("tensor"), lax.axis_size("context"))
    X, Z, ZL = grid.X, grid.Z, grid.ZL
    place = lax.axis_index("context")
    z, x = place // X, place % X
    half, low = z // ZL, z % ZL
    spans, select = selected.shape
    rows = tokens.shape[0]
    span_rows = rows // spans
    capacity = max(GROUP, 2 * spans * select // grid.C)
    table, item_count = work_table(
        selected, counts, block_slot, cache_keys.shape[0], capacity, place
    )

    query_blocks = gather_weight(grid, query_weight)
    order = list(query_blocks)
    whole = spread_tokens(grid, tokens)
    depth = query_weight.shape[0]

    def features_of(which):
        return [
            lax.dynamic_slice(
                whole,
                (which, 0, ((low - dz) % ZL * X + (x - dx) % X) * depth),
                (1, rows, depth),
            )[0]
            for dz, dx in order
        ]

    other_features, own_features = features_of(1 - half), features_of(half)

    def product(blocks, features, out_type):
        return project(features, [blocks[key] for key in order], out_type)

    sent = product(query_blocks, other_features, jnp.float32)
    arrived = grid.swap_half(sent)
    kept = product(query_blocks, own_features, jnp.float32)
    queries = (kept + arrived).astype(jnp.bfloat16)

    def narrow_project(weight, after):
        weight, _ = lax.optimization_barrier((weight, after))
        blocks = gather_weight(grid, weight)
        there = product(blocks, other_features, jnp.bfloat16)
        here = product(blocks, own_features, jnp.float32)
        back = grid.swap_half(there)
        return (here + back.astype(jnp.float32)).astype(jnp.bfloat16)

    new_keys = narrow_project(key_weight, sent)

    by_z = [queries] + [grid.shift_z(queries, k) for k in range(1, Z)]
    merged = []
    for k in range(Z):
        partials = {}
        for dx in list(range(1, X)) + [0]:
            asked = grid.shift_x(by_z[k], dx) if dx else by_z[k]
            source = grid.at(z - k, x - dx).astype(jnp.int32).reshape(1)
            partials[dx] = far_partial(
                asked, source, table, item_count, cache_keys, cache_values, span_rows
            )
        together = [partials[0]] + [grid.shift_x(partials[dx], -dx) for dx in range(1, X)]
        merged.append(merge(together, True) if X > 1 else together[0])
    returned = [merged[0]] + [grid.shift_z(merged[k], -k) for k in range(1, Z)]

    new_values = narrow_project(value_weight, queries)
    ends = jnp.stack([new_keys[rows - span_rows :], new_values[rows - span_rows :]])
    prior = lax.ppermute(ends, "context", [(i - 1, i) for i in range(1, grid.C)])
    first = jnp.where(place == 0, span_rows, 0).astype(jnp.int32).reshape(1)
    near = near_partial(queries, new_keys, new_values, prior[0], prior[1], first)
    return merge(returned + [near], False)


def solution(mesh):
    placed = (
        P("context", "tensor"),
        P("context", "tensor"),
        P("context", "tensor"),
        P("context", "tensor"),
        P("context", None, "tensor"),
        P("context", None, "tensor"),
        P("context", None),
        P("context"),
        P(),
    )
    return jax.shard_map(
        shards, mesh=mesh, in_specs=placed, out_specs=P("context", "tensor"), check_vma=False
    )
```
